32 devices in a mesh: dp: 4 (over x, y), sp: 8 (over z, core).
Axes of the slice: x: 2, y: 2, z: 4, core: 2. Of those that a mesh axis runs over, the one named last changes fastest.
Arguments:
- x: bfloat16 [8192, 7168], P(('dp', 'sp')), parts along dimension 0
- gain: bfloat16 [7168], replicated
- wq: bfloat16 [7168, 7168], replicated
- wk: bfloat16 [7168, 1024], replicated
- wv: bfloat16 [7168, 1024], replicated
- wo: bfloat16 [7168, 7168], replicated
Outputs:
- output: bfloat16 [8192, 7168], P(('dp', 'sp')), parts along dimension 0
There are 4 independent parts. The reference program is written for one: setup_inputs(seed, part) draws one part's arguments, and reference() takes and returns one part's arrays. A program takes and returns all parts, laid end to end along the dimension named above; an argument that names none is the same for every part.
All inputs are finite; a program needn't handle non-finite values.
Results may differ from the reference program's by a relative error of at most 0.012.
Values are sent between devices in bfloat16 or wider.
A program may use at most 2 GiB of HBM per device.

```python
import jax
import jax.numpy as jnp
from jax import lax

ROWS = 2048
D = 7168
HEADS = 56
KV_HEADS = 8
HEAD = 128
THETA = 10000


def setup_inputs(seed: int = 0, part: int = 0) -> dict:
    kx, kn, kq, kk, kv, ko = jax.random.split(jax.random.key(seed), 6)

    def weights(key, rows, columns):
        return jax.random.normal(key, (rows, columns), jnp.float32) * rows**-0.5

    drawn = {
        "x": jax.random.normal(jax.random.fold_in(kx, part), (ROWS, D), jnp.float32),
        "gain": 1 + 0.1 * jax.random.normal(kn, (D,), jnp.float32),
        "wq": 2 * weights(kq, D, HEADS * HEAD),
        "wk": 2 * weights(kk, D, KV_HEADS * HEAD),
        "wv": 4 * weights(kv, D, KV_HEADS * HEAD),
        "wo": weights(ko, HEADS * HEAD, D),
    }
    return {k: v.astype(jnp.bfloat16) for k, v in drawn.items()}


def normed(x, gain):
    wide = x.astype(jnp.float32)
    scale = lax.rsqrt(jnp.mean(wide * wide, -1, keepdims=True) + 1e-6)
    return (wide * scale * gain.astype(jnp.float32)).astype(jnp.bfloat16)


def turned(t, place, theta):
    half = t.shape[-1] // 2
    angle = place.astype(jnp.float32)[:, None] * theta ** (-jnp.arange(half, dtype=jnp.float32) / half)
    cos, sin = jnp.cos(angle)[:, None], jnp.sin(angle)[:, None]
    a, b = t[..., :half].astype(jnp.float32), t[..., half:].astype(jnp.float32)
    return jnp.concatenate([a * cos - b * sin, b * cos + a * sin], -1).astype(jnp.bfloat16)


def matmul(a, w):
    return jnp.dot(a, w, preferred_element_type=jnp.float32).astype(jnp.bfloat16)


def einsum(form, a, b):
    return jnp.einsum(form, a.astype(jnp.float32), b.astype(jnp.float32))


def attention(q, k, v):
    scores = einsum("tgsd,ugd->gstu", q, k) * q.shape[-1] ** -0.5
    token = jnp.arange(q.shape[0])
    scores = jnp.where(token[:, None] >= token, scores, -jnp.inf)
    weights = jax.nn.softmax(scores, -1).astype(jnp.bfloat16)
    return einsum("gstu,ugd->tgsd", weights, v).astype(jnp.bfloat16)


def reference(x, gain, wq, wk, wv, wo):
    a, place = normed(x, gain), jnp.arange(ROWS)
    q = turned(matmul(a, wq).reshape(ROWS, HEADS, HEAD), place, THETA).reshape(ROWS, KV_HEADS, -1, HEAD)
    k = turned(matmul(a, wk).reshape(ROWS, KV_HEADS, HEAD), place, THETA)
    v = matmul(a, wv).reshape(ROWS, KV_HEADS, HEAD)
    seen = attention(q, k, v).reshape(ROWS, HEADS * HEAD)
    return (x.astype(jnp.float32) + jnp.dot(seen, wo, preferred_element_type=jnp.float32)).astype(jnp.bfloat16)
```

```python
import functools

import jax
import jax.numpy as jnp
from jax import lax
from jax.experimental import pallas as pl
from jax.experimental.pallas import tpu as pltpu
from jax.sharding import PartitionSpec as P

HEAD = 128
THETA = 10000
NEG = -1e30
HIDDEN = 2 * NEG
LOG2E = 1.4426950408889634
TILE = 512
SLOTS = 3
MESH = pl.DeviceIdType.MESH


def _dot(a, b, ca=1, cb=0):
    return lax.dot_general(a, b, (((ca,), (cb,)), ((), ())), preferred_element_type=jnp.float32)


def _kernel(chips, kvh, grp, x_ref, gain_ref, cos_ref, sin_ref, wq_ref, wk_ref, wv_ref, wo_ref, y_ref,
            a_s, w_s, q_s, kv_s, top_s, mix_s, o_s, osend_s, y_s,
            w_sem, x_sem, xs_sem, xr_sem, kvs_sem, kvr_sem, os_sem, or_sem, y_sem):
    rows, d = x_ref.shape
    both = 2 * rows
    nq = kvh * grp * HEAD // TILE
    no = d // TILE
    half_cols = kvh * grp * HEAD
    per = TILE // HEAD
    me = lax.axis_index("sp")
    k, core = me // 2, lax.rem(me, 2)
    partner, up, down = 2 * k + 1 - core, me + 2, me - 2
    e = HEAD**-0.5 * LOG2E

    def weight(ref, column, slot):
        return pltpu.make_async_copy(ref.at[:, pl.ds(pl.multiple_of(column, TILE), TILE)], w_s.at[slot], w_sem.at[slot])

    own = pl.ds(pl.multiple_of(core * rows, rows), rows)
    x_in = pltpu.make_async_copy(x_ref, a_s.at[own], x_sem)
    x_in.start()
    weight(wk_ref, core * TILE, 0).start()
    weight(wv_ref, core * TILE, 1).start()
    weight(wq_ref, core * half_cols, 2).start()

    barrier = pltpu.get_barrier_semaphore()
    pl.semaphore_signal(barrier, inc=1, device_id={"sp": partner}, device_id_type=MESH)

    @pl.when(k < chips - 1)
    def _():
        pl.semaphore_signal(barrier, inc=1, device_id={"sp": up}, device_id_type=MESH)

    @pl.when(k > 0)
    def _():
        pl.semaphore_signal(barrier, inc=1, device_id={"sp": down}, device_id_type=MESH)

    pl.semaphore_wait(barrier, 1 + jnp.where(k < chips - 1, 1, 0) + jnp.where(k > 0, 1, 0))

    x_out = pltpu.make_async_remote_copy(src_ref=x_ref, dst_ref=a_s.at[own], send_sem=xs_sem, recv_sem=xr_sem,
                                         device_id={"sp": partner}, device_id_type=MESH)
    x_out.start()

    def kv_copy(c, g):
        return pltpu.make_async_remote_copy(src_ref=kv_s.at[c, g], dst_ref=kv_s.at[c, g], send_sem=kvs_sem.at[c, g],
                                            recv_sem=kvr_sem.at[c, g], device_id={"sp": up}, device_id_type=MESH)

    def turn(t, place):
        return (t * cos_ref[place, :] + pltpu.roll(t, HEAD // 2, 1) * sin_ref[place, :]).astype(jnp.bfloat16)

    def tokens(i, _):
        half = lax.rem(core + i, 2)
        here = pl.ds(pl.multiple_of(half * rows, rows), rows)

        @pl.when(i == 0)
        def _():
            x_in.wait()

        @pl.when(i == 1)
        def _():
            x_out.wait_recv()

        def norm(r, _):
            at = pl.ds(pl.multiple_of(half * rows + r * 16, 16), 16)
            wide = a_s[at, :].astype(jnp.float32)
            scale = lax.rsqrt(jnp.mean(wide * wide, -1, keepdims=True) + 1e-6)
            a_s[at, :] = (wide * scale * gain_ref[...].astype(jnp.float32)).astype(jnp.bfloat16)

        lax.fori_loop(0, rows // 16, norm, None)

        @pl.when(i == 0)
        def _():
            weight(wk_ref, core * TILE, 0).wait()
            weight(wv_ref, core * TILE, 1).wait()

        keys = _dot(a_s[here, :], w_s[0]).astype(jnp.bfloat16).astype(jnp.float32)
        for g in range(kvh):
            kv_s[k, g, 0, here, :] = turn(keys[:, g * HEAD : (g + 1) * HEAD], here)
        values = _dot(a_s[here, :], w_s[1]).astype(jnp.bfloat16)
        for g in range(kvh):
            kv_s[k, g, 1, here, :] = values[:, g * HEAD : (g + 1) * HEAD]

    lax.fori_loop(0, 2, tokens, None)
    weight(wq_ref, core * half_cols + TILE, 0).start()
    weight(wq_ref, core * half_cols + 2 * TILE, 1).start()

    @pl.when(k < chips - 1)
    def _():
        for g in range(kvh):
            kv_copy(k, g).start()

    everyone = pl.ds(0, both)

    def forward(c, g):
        kv_copy(c, g).wait_recv()
        kv_copy(c, g).start()

    def queries(i, _):
        slot = lax.rem(i + 2, SLOTS)
        weight(wq_ref, 0, slot).wait()
        t = _dot(a_s[...], w_s[slot]).astype(jnp.bfloat16).astype(jnp.float32)
        for h in range(per):
            q_s[i * per + h] = turn(t[:, h * HEAD : (h + 1) * HEAD], everyone)

        @pl.when(i + SLOTS < nq)
        def _():
            weight(wq_ref, core * half_cols + (i + SLOTS) * TILE, slot).start()

        @pl.when((i + SLOTS >= nq) & (i + SLOTS - nq < no))
        def _():
            weight(wo_ref, (i + SLOTS - nq) * TILE, slot).start()

        @pl.when((i >= nq - kvh) & (k > 0) & (k < chips - 1))
        def _():
            forward(k - 1, i - (nq - kvh))

    lax.fori_loop(0, nq, queries, None)
    x_out.wait_send()
    x_again = pltpu.make_async_copy(x_ref, a_s.at[pl.ds(0, rows)], x_sem)
    x_again.start()

    def block(c, g, masked, first):
        kk = kv_s[c, g, 0]
        scores = [_dot(kk, q_s[g * grp + i], 1, 1) for i in range(grp)]
        values = jnp.concatenate([kv_s[c, g, 1].T, jnp.ones((8, both), jnp.bfloat16)], axis=0)
        if masked:
            ok = lax.broadcasted_iota(jnp.int32, (both, both), 1) >= lax.broadcasted_iota(jnp.int32, (both, both), 0)
        weights, keeps = [], []
        for i, s in enumerate(scores):
            if masked:
                s = jnp.where(ok, s, HIDDEN)
            top = s.max(axis=0, keepdims=True)
            if not first:
                old = top_s[g, i : i + 1, :]
                top = jnp.maximum(old, top)
                keeps.append(jnp.exp2((old - top) * e))
            top_s[g, i : i + 1, :] = top
            weights.append(jnp.exp2((s - top) * e).astype(jnp.bfloat16))
        for i, p in enumerate(weights):
            part = _dot(values, p)
            h = g * grp + i
            mix_s[h] = part if first else mix_s[h] * keeps[i] + part

    def diagonal(g, _):
        block(k, g, True, True)

    lax.fori_loop(0, kvh, diagonal, None)

    def earlier(n, _):
        c, g = k - 1 - n // kvh, lax.rem(n, kvh)

        @pl.when(k == chips - 1)
        def _():
            kv_copy(c, g).wait_recv()

        @pl.when((k < chips - 1) & (c > 0))
        def _():
            forward(c - 1, g)

        block(c, g, False, False)

    lax.fori_loop(0, kvh * k, earlier, None)

    def o_copy(g):
        at = pl.ds(pl.multiple_of(g * grp * HEAD, HEAD), grp * HEAD)
        return pltpu.make_async_remote_copy(src_ref=osend_s.at[:, at], dst_ref=o_s.at[core, :, at], send_sem=os_sem.at[g],
                                            recv_sem=or_sem.at[g], device_id={"sp": partner}, device_id_type=MESH)

    own_first = pl.ds(pl.multiple_of(core * rows, rows), rows)
    other_first = pl.ds(pl.multiple_of((1 - core) * rows, rows), rows)

    def finish(g, _):
        for i in range(grp):
            h = g * grp + i
            at = pl.ds(pl.multiple_of(h * HEAD, HEAD), HEAD)
            for where, ref in ((other_first, osend_s), (own_first, o_s.at[core])):
                out = mix_s[h, :HEAD, where] * (1 / mix_s[h, HEAD : HEAD + 1, where])
                ref[:, at] = out.T.astype(jnp.bfloat16)
        o_copy(g).start()

    lax.fori_loop(0, kvh, finish, None)
    for g in range(kvh):
        o_copy(g).wait()
    x_again.wait()

    def y_copy(n, slot):
        return pltpu.make_async_copy(y_s.at[slot], y_ref.at[:, pl.ds(pl.multiple_of(n * TILE, TILE), TILE)], y_sem.at[slot])

    def project(n, _):
        slot, out = lax.rem(nq + 2 + n, SLOTS), lax.rem(n, 2)
        weight(wo_ref, 0, slot).wait()
        y = _dot(o_s[0], w_s[slot, :half_cols, :]) + _dot(o_s[1], w_s[slot, half_cols:, :])

        @pl.when(n >= 2)
        def _():
            y_copy(n - 2, out).wait()

        at = pl.ds(pl.multiple_of(n * TILE, TILE), TILE)
        y_s[out] = (a_s[pl.ds(0, rows), at].astype(jnp.float32) + y).astype(jnp.bfloat16)
        y_copy(n, out).start()

        @pl.when(n + SLOTS < no)
        def _():
            weight(wo_ref, (n + SLOTS) * TILE, slot).start()

    lax.fori_loop(0, no, project, None)
    for n in range(max(no - 2, 0), no):
        y_copy(n, n % 2).wait()

    @pl.when(k < chips - 1)
    def _():
        def sent(n, _):
            kv_copy(n // kvh, lax.rem(n, kvh)).wait_send()

        lax.fori_loop(0, kvh * (k + 1), sent, None)


def solution(mesh):
    chips = mesh.shape["sp"] // 2

    def step(x, gain, wq, wk, wv, wo):
        rows, d = x.shape
        kvh = wk.shape[1] // HEAD // 2
        grp = wq.shape[1] // wk.shape[1]
        heads, half = kvh * grp, HEAD // 2
        place = (lax.axis_index("sp") // 2 * 2 * rows + jnp.arange(2 * rows)).astype(jnp.float32)
        angle = place[:, None] * THETA ** (-jnp.arange(half, dtype=jnp.float32) / half)
        cos, sin = jnp.cos(angle), jnp.sin(angle)
        cos, sin = jnp.concatenate([cos, cos], 1), jnp.concatenate([-sin, sin], 1)
        anywhere, vmem = pl.BlockSpec(memory_space=pl.ANY), pl.BlockSpec(memory_space=pltpu.VMEM)
        dma = pltpu.SemaphoreType.DMA
        return pl.pallas_call(
            functools.partial(_kernel, chips, kvh, grp),
            out_shape=jax.ShapeDtypeStruct((rows, d), jnp.bfloat16),
            in_specs=[anywhere, vmem, vmem, vmem, anywhere, anywhere, anywhere, anywhere],
            out_specs=anywhere,
            scratch_shapes=[
                pltpu.VMEM((2 * rows, d), jnp.bfloat16),
                pltpu.VMEM((SLOTS, d, TILE), jnp.bfloat16),
                pltpu.VMEM((heads, 2 * rows, HEAD), jnp.bfloat16),
                pltpu.VMEM((chips, kvh, 2, 2 * rows, HEAD), jnp.bfloat16),
                pltpu.VMEM((kvh, 8, 2 * rows), jnp.float32),
                pltpu.VMEM((heads, HEAD + 8, 2 * rows), jnp.float32),
                pltpu.VMEM((2, rows, heads * HEAD), jnp.bfloat16),
                pltpu.VMEM((rows, heads * HEAD), jnp.bfloat16),
                pltpu.VMEM((2, rows, TILE), jnp.bfloat16),
                dma((SLOTS,)), dma, dma, dma, dma((chips, kvh)), dma((chips, kvh)), dma((kvh,)), dma((kvh,)), dma((2,)),
            ],
            compiler_params=pltpu.CompilerParams(collective_id=0, has_side_effects=True, vmem_limit_bytes=67043328),
            name="layer",
        )(x, gain[None], cos, sin, wq, wk, wv, wo)

    tokens, whole = P(("dp", "sp"), None), P(None, None)
    return jax.shard_map(
        step,
        mesh=mesh,
        in_specs=(tokens, P(None), whole, whole, whole, whole),
        out_specs=tokens,
        check_vma=False,
    )
```

```python
import functools

import jax
import jax.numpy as jnp
import numpy as np
from jax import lax
from jax.experimental import pallas as pl
from jax.experimental.pallas import tpu as pltpu
from jax.sharding import PartitionSpec as P

HEAD = 128
THETA = 10000
NEG = -1e30
HIDDEN = 2 * NEG
LOG2E = 1.4426950408889634
TILE = 512
NORM = 32
SLOTS = 3
MESH = pl.DeviceIdType.MESH


def _dot(a, b, ca=1, cb=0):
    return lax.dot_general(a, b, (((ca,), (cb,)), ((), ())), preferred_element_type=jnp.float32)


def _kernel(chips, kvh, grp, x_ref, gain_ref, freq_ref, wq_ref, wk_ref, wv_ref, wo_ref, y_ref,
            a_s, w_s, q_s, kv_s, kvx_s, top_s, mix_s, o_s, sum_s, cos_s, sin_s, gain_s,
            w_sem, x_sem, as_sem, ar_sem, us_sem, ur_sem, ps_sem, pr_sem, kvs_sem, kvr_sem, os_sem, or_sem, y_sem):
    rows, d = x_ref.shape
    both = 2 * rows
    nq = kvh * grp * HEAD // TILE
    no = d // (2 * TILE)
    half_cols = kvh * grp * HEAD
    per = TILE // HEAD
    me = lax.axis_index("sp")
    k, core = me // 2, lax.rem(me, 2)
    partner, up = 2 * k + 1 - core, me + 2
    e = HEAD**-0.5 * LOG2E


    def weight(ref, column, slot):
        return pltpu.make_async_copy(ref.at[:, :, :, pl.ds(pl.multiple_of(column, TILE), TILE)], w_s.at[slot], w_sem.at[slot, 0])

    def result_weight(u, j, slot):
        at = pl.ds(pl.multiple_of((2 * lax.rem(u, no) + j) * TILE, TILE), TILE)
        return pltpu.make_async_copy(wo_ref.at[:, u // no, :, at], w_s.at[slot, j], w_sem.at[slot, j])

    def remote(src, dst, send, recv, device):
        return pltpu.make_async_remote_copy(src_ref=src, dst_ref=dst, send_sem=send, recv_sem=recv, device_id={"sp": device},
                                            device_id_type=MESH)

    own = pl.ds(pl.multiple_of(core * rows, rows), rows)
    everyone = pl.ds(0, both)
    part = rows // 2

    def x_in(i):
        at = pl.ds(i * part, part)
        return pltpu.make_async_copy(x_ref.at[at], a_s.at[pl.ds(pl.multiple_of(core * rows + i * part, part), part)], x_sem.at[i])

    x_in(0).start()
    x_in(1).start()

    barrier = pltpu.get_barrier_semaphore()
    pl.semaphore_signal(barrier, inc=1, device_id={"sp": partner}, device_id_type=MESH)

    @pl.when(k < chips - 1)
    def _():
        for c in range(2):
            pl.semaphore_signal(barrier, inc=1, device_id={"sp": 2 * k + 2 + c}, device_id_type=MESH)

    @pl.when(k > 0)
    def _():
        for c in range(2):
            pl.semaphore_signal(barrier, inc=1, device_id={"sp": 2 * k - 2 + c}, device_id_type=MESH)

    weight(wk_ref, core * TILE, 0).start()
    for j in range(d // HEAD):
        gain_s[:, j * HEAD : (j + 1) * HEAD] = gain_ref[j : j + 1, :].astype(jnp.float32)
    place = (lax.broadcasted_iota(jnp.int32, (both, HEAD), 0) + k * both).astype(jnp.float32)
    angle = place * freq_ref[...]
    cos_s[...] = jnp.cos(angle)
    sine = jnp.sin(angle)
    sin_s[...] = jnp.where(lax.broadcasted_iota(jnp.int32, (both, HEAD), 1) < HEAD // 2, -sine, sine)

    pl.semaphore_wait(barrier, 1 + jnp.where(k < chips - 1, 2, 0) + jnp.where(k > 0, 2, 0))

    def a_copy(i):
        at = pl.ds(pl.multiple_of(core * rows + i * part, part), part)
        return remote(a_s.at[at], a_s.at[at], as_sem.at[i], ar_sem.at[i], partner)

    step = min(NORM, part)
    for i in range(2):
        x_in(i).wait()

        def norm(r, _):
            at = pl.ds(pl.multiple_of(core * rows + i * part + r * step, step), step)
            wide = a_s[at, :].astype(jnp.float32)
            scale = lax.rsqrt(jnp.mean(wide * wide, -1, keepdims=True) + 1e-6)
            a_s[at, :] = (wide * scale * gain_s[...]).astype(jnp.bfloat16)

        lax.fori_loop(0, part // step, norm, None)
        if i == 0:
            weight(wv_ref, core * TILE, 1).start()
    a_copy(0).start()
    weight(wk_ref, (1 - core) * TILE, 2).start()

    def turn(t, place):
        return (t * cos_s[place, :] + pltpu.roll(t, HEAD // 2, 1) * sin_s[place, :]).astype(jnp.bfloat16)

    def up_copy(i, t):
        return remote(kvx_s.at[t] if i else kv_s.at[k, :, t, own], kv_s.at[k, :, t, own], us_sem.at[i, t], ur_sem.at[core, t],
                      2 * k + 2 + (1 - core if i else core))

    def side_copy(t):
        return remote(kvx_s.at[t], kv_s.at[k, :, t, own], ps_sem.at[t], pr_sem.at[t], partner)

    def keys_values(i, _):
        for t, ref in ((0, wk_ref), (1, wv_ref)):
            slot = lax.rem(2 * i + t, SLOTS)
            weight(ref, 0, slot).wait()
            if t == 0:

                @pl.when(i == 1)
                def _():
                    weight(wq_ref, core * half_cols, 1).start()

            out = _dot(a_s[own, :], w_s[slot].reshape(d, TILE)).astype(jnp.bfloat16)
            if t == 0:
                out = out.astype(jnp.float32)
            for g in range(kvh):
                piece = out[:, g * HEAD : (g + 1) * HEAD]
                if t == 0:
                    piece = turn(piece, own)

                @pl.when(i == 0)
                def _():
                    kv_s[k, g, t, own, :] = piece

                @pl.when(i == 1)
                def _():
                    kvx_s[t, g] = piece

            for n in range(2):

                @pl.when((k < chips - 1) & (i == n))
                def _():
                    up_copy(n, t).start()

            @pl.when(i == 1)
            def _():
                side_copy(t).start()

            if t == 0:

                @pl.when(i == 0)
                def _():
                    a_copy(1).start()
                    weight(wv_ref, (1 - core) * TILE, 0).start()

                @pl.when(i == 1)
                def _():
                    weight(wq_ref, core * half_cols + TILE, 2).start()

    lax.fori_loop(0, 2, keys_values, None)
    weight(wq_ref, core * half_cols + 2 * TILE, 0).start()
    for i in range(2):
        a_copy(i).wait_recv()

    def kv_copy(c, g):
        return remote(kv_s.at[c, g], kv_s.at[c, g], kvs_sem.at[c, g], kvr_sem.at[c, g], up)

    def arrived():
        for c in range(2):
            for t in range(2):
                at = kv_s.at[k - 1, :, t, pl.ds(c * rows, rows)]
                remote(at, at, us_sem.at[0, t], ur_sem.at[c, t], partner).wait_recv()

    def pass_on(c, g):
        kv_copy(c, g).wait_recv()
        kv_copy(c, g).start()

    def queries(i, _):
        slot = lax.rem(i + 1, SLOTS)
        weight(wq_ref, 0, slot).wait()
        for at in (pl.ds(0, rows), pl.ds(rows, rows)):
            t = _dot(a_s[at, :], w_s[slot].reshape(d, TILE)).astype(jnp.bfloat16).astype(jnp.float32)
            for h in range(per):
                q_s[i * per + h, at, :] = turn(t[:, h * HEAD : (h + 1) * HEAD], at)

        @pl.when(i + SLOTS < nq)
        def _():
            weight(wq_ref, core * half_cols + (i + SLOTS) * TILE, slot).start()

        @pl.when(i + SLOTS >= nq)
        def _():
            for j in range(2):
                result_weight(i + SLOTS - nq, j, slot).start()

        @pl.when((k == 1) & (i == nq // 2))
        def _():
            arrived()
            for g in range(kvh):
                kv_copy(0, g).start()

        @pl.when((k == 2) & (i == nq // 2))
        def _():
            arrived()
            for g in range(2):
                kv_copy(1, g).start()

        @pl.when((k == 2) & (i == nq - 2))
        def _():
            pass_on(0, 0)

    lax.fori_loop(0, nq, queries, None)

    @pl.when(k == 2)
    def _():
        pass_on(0, 1)
        kv_copy(1, 2).start()

    @pl.when(k == 3)
    def _():
        arrived()

    for i in range(2):
        a_copy(i).wait_send()
    x_again = pltpu.make_async_copy(x_ref, a_s.at[pl.ds(rows, rows)], x_sem.at[0])
    x_again.start()
    for t in range(2):
        at = kv_s.at[k, :, t, pl.ds(pl.multiple_of((1 - core) * rows, rows), rows)]
        remote(at, at, ps_sem.at[t], pr_sem.at[t], partner).wait_recv()

    def diagonal(g):
        kk = kv_s[k, g, 0]
        early = [_dot(kk[:rows], q_s[g * grp + i], 1, 1) for i in range(grp)]
        late = [_dot(kk[rows:], q_s[g * grp + i, rows:, :], 1, 1) for i in range(grp)]
        values = jnp.concatenate([kv_s[k, g, 1].T, jnp.ones((8, both), jnp.bfloat16)], axis=0)
        ok = lax.broadcasted_iota(jnp.int32, (rows, rows), 1) >= lax.broadcasted_iota(jnp.int32, (rows, rows), 0)
        weights = []
        for i in range(grp):
            s, r, t = jnp.where(ok, early[i][:, :rows], HIDDEN), early[i][:, rows:], jnp.where(ok, late[i], HIDDEN)
            top = s.max(axis=0, keepdims=True)
            top_s[i : i + 1, :rows] = top
            s = jnp.exp2((s - top) * e).astype(jnp.bfloat16)
            top = jnp.maximum(r.max(axis=0, keepdims=True), t.max(axis=0, keepdims=True))
            top_s[i : i + 1, rows:] = top
            weights.append((s, jnp.exp2((r - top) * e).astype(jnp.bfloat16), jnp.exp2((t - top) * e).astype(jnp.bfloat16)))
        for i, (s, r, t) in enumerate(weights):
            mix_s[i, :, :rows] = _dot(values[:, :rows], s)
            mix_s[i, :, rows:] = _dot(values, jnp.concatenate([r, t], axis=0))

    def block(c, g):
        kk = kv_s[c, g, 0]
        values = jnp.concatenate([kv_s[c, g, 1].T, jnp.ones((8, both), jnp.bfloat16)], axis=0)
        for some in (range(grp // 2 + 1), range(grp // 2 + 1, grp)):
            scores = [_dot(kk, q_s[g * grp + i], 1, 1) for i in some]
            weights, keeps = [], []
            for i, s in zip(some, scores):
                old = top_s[i : i + 1, :]
                top = jnp.maximum(old, s.max(axis=0, keepdims=True))
                keeps.append(jnp.exp2((old - top) * e))
                top_s[i : i + 1, :] = top
                weights.append(jnp.exp2((s - top) * e).astype(jnp.bfloat16))
            for i, p, keep in zip(some, weights, keeps):
                mix_s[i] = mix_s[i] * keep + _dot(values, p)

    width = grp * HEAD
    other = pl.ds(pl.multiple_of((1 - core) * rows, rows), rows)

    def o_copy(ph, g):
        at = pl.ds(pl.multiple_of((2 * ph + g) * width, HEAD), width)
        to = pl.ds(pl.multiple_of(g * width, HEAD), width)
        return remote(a_s.at[pl.ds(0, rows), at], o_s.at[ph, core, :, to], os_sem.at[ph, g], or_sem.at[ph, g], partner)

    def head(g, _):
        ph, n = g // 2, lax.rem(g, 2)

        @pl.when((k == 2) & (g == 1))
        def _():
            pass_on(0, 2)
            kv_copy(1, 3).start()

        @pl.when((k == 2) & (g == 2))
        def _():
            pass_on(0, 3)

        diagonal(g)

        def earlier(j, _):
            c = k - 1 - j

            @pl.when((k == 3) & (j > 0))
            def _():
                kv_copy(c, g).wait_recv()

            block(c, g)

        lax.fori_loop(0, k, earlier, None)
        for i in range(grp):
            at = pl.ds(pl.multiple_of(n * width + i * HEAD, HEAD), HEAD)
            out = mix_s[i, :HEAD, other] * (1 / mix_s[i, HEAD : HEAD + 1, other])
            a_s[pl.ds(0, rows), pl.ds(pl.multiple_of(g * width + i * HEAD, HEAD), HEAD)] = out.T.astype(jnp.bfloat16)
            out = mix_s[i, :HEAD, own] * (1 / mix_s[i, HEAD : HEAD + 1, own])
            o_s[ph, core, :, at] = out.T.astype(jnp.bfloat16)
        o_copy(ph, n).start()

    def exchanged(ph):
        for g in range(2):
            o_copy(ph, g).wait()

    def y_copy(n):
        at = pl.ds(pl.multiple_of(n * 2 * TILE, TILE), 2 * TILE)
        return pltpu.make_async_copy(a_s.at[pl.ds(rows, rows), at], y_ref.at[:, at], y_sem.at[n])

    def project(ph, n):
        u = ph * no + n
        slot = lax.rem(nq + 1 + u, SLOTS)
        for j in range(2):
            result_weight(0, j, slot).wait()
        for j in range(2):
            at = pl.ds(pl.multiple_of((2 * n + j) * TILE, TILE), TILE)
            y = _dot(o_s[ph, 0], w_s[slot, j, 0]) + _dot(o_s[ph, 1], w_s[slot, j, 1])
            if ph == 0:
                sum_s[:, at] = y
            else:
                here = pl.ds(rows, rows)
                a_s[here, at] = (a_s[here, at].astype(jnp.float32) + (sum_s[:, at] + y)).astype(jnp.bfloat16)

        if ph == 1:
            y_copy(n).start()

        @pl.when(u + SLOTS < 2 * no)
        def _():
            for j in range(2):
                result_weight(u + SLOTS, j, slot).start()

    lax.fori_loop(0, 3, head, None)
    exchanged(0)
    first = no // 2
    lax.fori_loop(0, first, lambda n, _: project(0, n), None)
    lax.fori_loop(3, 4, head, None)
    lax.fori_loop(first, no, lambda n, _: project(0, n), None)
    exchanged(1)
    x_again.wait()
    lax.fori_loop(0, no, lambda n, _: project(1, n), None)
    for n in range(no):
        y_copy(n).wait()

    for t in range(2):
        side_copy(t).wait_send()

    @pl.when(k < chips - 1)
    def _():
        for i in range(2):
            for t in range(2):
                up_copy(i, t).wait_send()

        def sent(n, _):
            kv_copy(n // kvh, lax.rem(n, kvh)).wait_send()

        lax.fori_loop(0, kvh * k, sent, None)


def solution(mesh):
    chips = mesh.shape["sp"] // 2

    def step(x, gain, wq, wk, wv, wo):
        rows, d = x.shape
        kvh = wk.shape[1] // HEAD // 2
        grp = wq.shape[1] // wk.shape[1]
        heads, half = kvh * grp, HEAD // 2
        freq = np.float32(THETA) ** (-np.arange(half, dtype=np.float32) / np.float32(half))
        freq = jnp.asarray(np.concatenate([freq, freq])[None])
        anywhere, vmem = pl.BlockSpec(memory_space=pl.ANY), pl.BlockSpec(memory_space=pltpu.VMEM)
        dma = pltpu.SemaphoreType.DMA
        return pl.pallas_call(
            functools.partial(_kernel, chips, kvh, grp),
            out_shape=jax.ShapeDtypeStruct((rows, d), jnp.bfloat16),
            in_specs=[anywhere, vmem, vmem, anywhere, anywhere, anywhere, anywhere],
            out_specs=anywhere,
            scratch_shapes=[
                pltpu.VMEM((2 * rows, d), jnp.bfloat16),
                pltpu.VMEM((SLOTS, 2, 2, d // 4, TILE), jnp.bfloat16),
                pltpu.VMEM((heads, 2 * rows, HEAD), jnp.bfloat16),
                pltpu.VMEM((chips, kvh, 2, 2 * rows, HEAD), jnp.bfloat16),
                pltpu.VMEM((2, kvh, rows, HEAD), jnp.bfloat16),
                pltpu.VMEM((8, 2 * rows), jnp.float32),
                pltpu.VMEM((grp, HEAD + 8, 2 * rows), jnp.float32),
                pltpu.VMEM((2, 2, rows, heads * HEAD // 2), jnp.bfloat16),
                pltpu.VMEM((rows, d), jnp.float32),
                pltpu.VMEM((2 * rows, HEAD), jnp.float32),
                pltpu.VMEM((2 * rows, HEAD), jnp.float32),
                pltpu.VMEM((1, d), jnp.float32),
                dma((SLOTS, 2)), dma((2,)), dma((2,)), dma((2,)), dma((2, 2)), dma((2, 2)), dma((2,)), dma((2,)),
                dma((chips, kvh)), dma((chips, kvh)), dma((2, 2)), dma((2, 2)), dma((d // (2 * TILE),)),
            ],
            compiler_params=pltpu.CompilerParams(collective_id=0, has_side_effects=True, vmem_limit_bytes=67043328),
            name="layer",
        )(x, gain.reshape(-1, HEAD), freq, *(w.reshape(2, 2, d // 4, -1) for w in (wq, wk, wv, wo)))

    tokens, whole = P(("dp", "sp"), None), P(None, None)
    return jax.shard_map(
        step,
        mesh=mesh,
        in_specs=(tokens, P(None), whole, whole, whole, whole),
        out_specs=tokens,
        check_vma=False,
    )
```
